32 devices in a mesh: dp: 4 (over z), tensor: 8 (over y, x, core).
Axes of the slice: x: 2, y: 2, z: 4, core: 2. Of those that a mesh axis runs over, the one named last changes fastest.
Arguments:
- layer_input: bfloat16 [16384, 2048], P(('dp', 'tensor')), may hold values from -20 to 20
- gain_attn: float32 [2048], replicated, may hold values from 0.25 to 1.75
- w_query: bfloat16 [2048, 2048], P(None, 'tensor'), may hold values from -0.125 to 0.125
- w_key: bfloat16 [2048, 2048], P(None, 'tensor'), may hold values from -0.125 to 0.125
- w_value: bfloat16 [2048, 2048], P(None, 'tensor'), may hold values from -0.125 to 0.125
- w_out: bfloat16 [2048, 2048], P('tensor'), may hold values from -1 to 1
- gain_mlp: float32 [2048], replicated, may hold values from 0.25 to 1.75
- w_gate: bfloat16 [2048, 8192], P(None, 'tensor'), may hold values from -0.125 to 0.125
- w_up: bfloat16 [2048, 8192], P(None, 'tensor'), may hold values from -0.125 to 0.125
- w_down: bfloat16 [8192, 2048], P('tensor'), may hold values from -0.0625 to 0.0625
- segment_ids: int32 [8, 2048], P('dp'), may hold values from 0 to 31, as said below
- positions: int32 [8, 2048], P('dp'), may hold values from 0 to 2047, as said below
- out_grad: bfloat16 [16384, 2048], P(('dp', 'tensor')), may hold values from -6 to 6
Outputs:
- layer_out: bfloat16 [16384, 2048], P(('dp', 'tensor'))
- input_grad: float32 [16384, 2048], P(('dp', 'tensor'))
- grad_gain_attn: float32 [2048], P('tensor')
- grad_w_query: float32 [2048, 2048], P(None, 'tensor')
- grad_w_key: float32 [2048, 2048], P(None, 'tensor')
- grad_w_value: float32 [2048, 2048], P(None, 'tensor')
- grad_w_out: float32 [2048, 2048], P('tensor')
- grad_gain_mlp: float32 [2048], P('tensor')
- grad_w_gate: float32 [2048, 8192], P(None, 'tensor')
- grad_w_up: float32 [2048, 8192], P(None, 'tensor')
- grad_w_down: float32 [8192, 2048], P('tensor')
The draws below stay inside these ranges and needn't reach their ends.
Inputs may be any that keep to these rules, and one draw needn't show every extreme that they name: `segment_ids`: within each row the document number is 0 at the first token and rises by 0 or 1 from one token to the next; a row holds 1 to 32 documents; the first row of the batch is one document and the last row holds 32. `positions`: A position is 0 where a row begins or the document number changes, else one more than the position before.
All inputs are finite; a program needn't handle non-finite values.
Results may differ from the reference program's by a relative error of at most 0.024.
Values may be sent and summed in bfloat16 or wider, within the bound.
A program may use at most 320 MiB of HBM per device.

```python
import math
import jax
import jax.numpy as jnp
from jax import lax

D = 2048
HEADS = 32
HD = 64
FF = 8192
LEN = 2048
NROWS = 8
TOKENS = 16384


def draw_layer_input(key, part):
    key_base, key_scale = jax.random.split(key, 2)
    base_draw = jax.random.normal(key_base, (TOKENS, D), jnp.float32)
    low_end = math.log(0.3)
    high_end = math.log(3.0)
    base_draw = jnp.clip(base_draw, -5.0, 5.0)
    row_scale = jnp.exp(jax.random.uniform(key_scale, (TOKENS, 1), jnp.float32, low_end, high_end))
    return (base_draw * row_scale).astype(jnp.bfloat16)


def segment_layout(key):
    layout_key = jax.random.fold_in(key, 11)
    key_count, key_places = jax.random.split(layout_key)
    most_docs = LEN // 64
    row_number = jnp.arange(NROWS, dtype=jnp.int32)[:, None]
    counts = jax.random.randint(key_count, (NROWS, 1), 1, most_docs + 1).astype(jnp.int32)
    counts = jnp.where(row_number == 0, 1, counts)
    counts = jnp.where(row_number == NROWS - 1, most_docs, counts).astype(jnp.int32)
    row_keys = jax.random.split(key_places, NROWS)
    ranks = jax.vmap(lambda one_key: jax.random.permutation(one_key, LEN - 1))(row_keys).astype(jnp.int32)
    inner_starts = ranks < counts - 1
    column = jnp.arange(LEN, dtype=jnp.int32)[None, :]
    starts = jnp.concatenate([jnp.ones((NROWS, 1), jnp.bool_), inner_starts], axis=1)
    segment = jnp.cumsum(starts.astype(jnp.int32), axis=1) - 1
    latest = lax.cummax(jnp.where(starts, column, 0), axis=1)
    return (segment.astype(jnp.int32), (column - latest).astype(jnp.int32))


def draw_segment_ids(key, part):
    return segment_layout(key)[0]


def draw_positions(key, part):
    return segment_layout(key)[1]


def levels(key, shape, cuts, low, largest):
    level, own = 1.0, jax.random.fold_in(key, 6)
    for axis_at, blocks in cuts:
        draws = jnp.exp(jax.random.uniform(jax.random.fold_in(own, axis_at), (blocks,), jnp.float32, low / len(cuts), largest / len(cuts)))
        level = level * jnp.repeat(draws, shape[axis_at] // blocks).reshape([-1 if axis == axis_at else 1 for axis in range(len(shape))])
    return level


def centred(key, dims, spread, limit, cuts=(), kind=jnp.bfloat16):
    values = jax.random.normal(key, dims, jnp.float32) * spread
    if len(cuts) > 0:
        values = levels(key, dims, cuts, -0.22, 0.18) * values
    return jnp.clip(values, min=-limit, max=limit).astype(kind)


def setup_inputs(seed: int = 0) -> dict:
    keys = jax.random.split(jax.random.key(seed), 14)
    return {
        "layer_input": draw_layer_input(jax.random.fold_in(keys[13], 71), 0),
        "gain_attn": jnp.clip(1.0 + 0.15 * jax.random.normal(keys[1], (D,), jnp.float32), 0.25, 1.75),
        "w_query": centred(keys[2], (D, HEADS * HD), D ** -0.5, 0.125, ((1, 8),)),
        "w_key": centred(keys[3], (D, HEADS * HD), D ** -0.5, 0.125, ((1, 8),)),
        "w_value": centred(keys[4], (D, HEADS * HD), D ** -0.5, 0.125, ((1, 8),)),
        "w_out": centred(keys[5], (HEADS * HD, D), (HEADS * HD // 64) ** -0.5, 1.0, ((0, 8),)),
        "gain_mlp": jnp.clip(1.0 + 0.15 * jax.random.normal(keys[6], (D,), jnp.float32), 0.25, 1.75),
        "w_gate": centred(keys[7], (D, FF), D ** -0.5, 0.125, ((1, 8),)),
        "w_up": centred(keys[8], (D, FF), D ** -0.5, 0.125, ((1, 8),)),
        "w_down": centred(keys[9], (FF, D), FF ** -0.5, 0.0625, ((0, 8),)),
        "segment_ids": draw_segment_ids(jax.random.fold_in(keys[13], 71), 0),
        "positions": draw_positions(jax.random.fold_in(keys[13], 71), 0),
        "out_grad": centred(keys[12], (TOKENS, D), 1.0, 6.0, ((0, 32),)),
    }


rope_theta = 130000.0
norm_eps = 1e-05
highest = lax.Precision.HIGHEST

@jax.custom_vjp
def low(v):
    return lax.optimization_barrier(v.astype(jnp.bfloat16)).astype(jnp.float32)

@jax.custom_vjp
def low_back(v):
    return v

def low_keep(v):
    return (low(v), None)

def low_pass(kept, grad):
    return (grad,)

def back_keep(v):
    return (v, None)

def back_low(kept, grad):
    return (low(grad),)
low.defvjp(low_keep, low_pass)
low_back.defvjp(back_keep, back_low)

def rotary_tables(position_list, head_size):
    half_dim = head_size // 2
    frequency = rope_theta ** (-(jnp.arange(half_dim, dtype=jnp.float32) * 2.0 / head_size))
    angles = position_list.astype(jnp.float32)[:, None] * frequency[None, :]
    cosine_table = jnp.concatenate([jnp.cos(angles), jnp.cos(angles)], axis=-1)[:, None, :]
    sine_table = jnp.concatenate([jnp.sin(angles), jnp.sin(angles)], axis=-1)[:, None, :]
    return (cosine_table, sine_table)

def rotate(inputs, cosine_table, sine_table):
    half_dim = inputs.shape[-1] // 2
    turned = jnp.concatenate([-inputs[..., half_dim:], inputs[..., :half_dim]], axis=-1)
    return inputs * cosine_table + turned * sine_table

def normalize(row_values):
    inverse = lax.rsqrt(lax.optimization_barrier(jnp.mean(row_values * row_values, axis=-1, keepdims=True)) + norm_eps)
    return row_values * inverse

def attend_row(queries, key_heads, value_heads, segment_row):
    length = queries.shape[0]
    block_len = min(512, length)
    per_row = length // block_len
    scale_factor = HD ** (-0.5)

    def one_block(block_data):
        query_block, first_row = block_data
        q_index = first_row + jnp.arange(block_len, dtype=jnp.int32)
        seg_query = lax.dynamic_slice_in_dim(segment_row, first_row, block_len)
        allowed = (seg_query[:, None] == segment_row[None, :]) & (jnp.arange(length, dtype=jnp.int32)[None, :] <= q_index[:, None])
        scores = jnp.einsum('qhd,khd->hqk', query_block, key_heads, precision=highest) * scale_factor
        scores = low_back(scores)
        scores = jnp.where(allowed[None], scores, -1e+30)
        probabilities = jax.nn.softmax(scores, axis=-1)
        mixed = jnp.einsum('hqk,khd->qhd', low(probabilities), value_heads, precision=highest)
        return low(low_back(mixed))
    blocks = queries.reshape(per_row, block_len, queries.shape[1], queries.shape[2])
    firsts = (jnp.arange(per_row, dtype=jnp.int32) * block_len).astype(jnp.int32)
    outputs = lax.map(jax.checkpoint(one_block), (blocks, firsts))
    return outputs.reshape(length, -1)

def layer_row(row_data, weight_tuple):
    row_input, segment_row, position_row = row_data
    gain_one, wq_full, wk_full, wv_full, wo_full, gain_two, wg_full, wu_full, wd_full = weight_tuple
    length = row_input.shape[0]
    normed_one = low(normalize(row_input) * gain_one)
    cosine_table, sine_table = rotary_tables(position_row, HD)
    query_pre = low_back(jnp.dot(normed_one, wq_full, precision=highest)).reshape(length, -1, HD)
    key_pre = low_back(jnp.dot(normed_one, wk_full, precision=highest)).reshape(length, -1, HD)
    value_pre = low_back(jnp.dot(normed_one, wv_full, precision=highest)).reshape(length, -1, HD)
    queries = low(rotate(query_pre, cosine_table, sine_table))
    key_heads = low(rotate(key_pre, cosine_table, sine_table))
    value_heads = low(value_pre)
    attended = attend_row(queries, key_heads, value_heads, segment_row)
    residual = row_input + low_back(jnp.dot(attended, wo_full, precision=highest))
    normed_two = low(normalize(residual) * gain_two)
    gate_pre = low_back(jnp.dot(normed_two, wg_full, precision=highest))
    up_pre = low_back(jnp.dot(normed_two, wu_full, precision=highest))
    hidden = low(jax.nn.silu(gate_pre) * up_pre)
    return residual + low_back(jnp.dot(hidden, wd_full, precision=highest))

def reference(layer_input, gain_attn, w_query, w_key, w_value, w_out, gain_mlp, w_gate, w_up, w_down, segment_ids, positions, out_grad):
    row_total = segment_ids.shape[0]
    length = segment_ids.shape[1]
    width = layer_input.shape[1]
    weight_tuple = (gain_attn.astype(jnp.float32), w_query.astype(jnp.float32), w_key.astype(jnp.float32), w_value.astype(jnp.float32), w_out.astype(jnp.float32), gain_mlp.astype(jnp.float32), w_gate.astype(jnp.float32), w_up.astype(jnp.float32), w_down.astype(jnp.float32))

    def forward(inputs, weights_now):

        def per_row(row_data):
            return layer_row(row_data, weights_now)
        stacked = lax.map(jax.checkpoint(per_row), (inputs.reshape(row_total, length, width), segment_ids, positions))
        return stacked.reshape(row_total * length, width)
    layer_value, pull_back = jax.vjp(forward, layer_input.astype(jnp.float32), weight_tuple)
    input_grad, weight_grads = pull_back(out_grad.astype(jnp.float32))
    return (layer_value.astype(jnp.bfloat16), input_grad, weight_grads[0], weight_grads[1], weight_grads[2], weight_grads[3], weight_grads[4], weight_grads[5], weight_grads[6], weight_grads[7], weight_grads[8])
```

```python
import functools
import jax
import jax.numpy as jnp
from jax import lax
from jax.experimental import pallas as pl
from jax.experimental.pallas import tpu as pltpu
from jax.sharding import PartitionSpec as P

HD = 64
NEG = -1e30
NT = (((1,), (1,)), ((), ()))
VMEM_MAX = 60 * 1024 * 1024


def swap_halves(values):
    width = values.shape[-1]
    if width == HD:
        return jnp.concatenate([values[:, HD // 2 :], values[:, : HD // 2]], axis=1)
    lane = lax.broadcasted_iota(jnp.int32, values.shape, 1)
    return jnp.where(
        lane % HD < HD // 2,
        pltpu.roll(values, width - HD // 2, 1),
        pltpu.roll(values, HD // 2, 1),
    )


def turn(values, cosine, sine):
    width = cosine.shape[-1]
    parts = []
    for start in range(0, values.shape[-1], width):
        piece = values[:, start : start + width]
        parts.append(piece * cosine + swap_halves(piece) * sine)
    return parts[0] if len(parts) == 1 else jnp.concatenate(parts, axis=1)


def turn_back(values, cosine, sine):
    width = cosine.shape[-1]
    parts = []
    for start in range(0, values.shape[-1], width):
        piece = values[:, start : start + width]
        parts.append(piece * cosine + swap_halves(piece * sine))
    return parts[0] if len(parts) == 1 else jnp.concatenate(parts, axis=1)


def qkv_kernel(x_ref, w_ref, cos_ref, sin_ref, q_ref, k_ref, v_ref):
    width = q_ref.shape[1]
    projected = jnp.dot(x_ref[...], w_ref[...], preferred_element_type=jnp.float32)
    cosine, sine = cos_ref[...], sin_ref[...]
    turned = turn(projected[:, :width], cosine, sine).astype(jnp.bfloat16)
    q_ref[...] = turned * jnp.bfloat16(HD**-0.5)
    k_ref[...] = turn(projected[:, width : 2 * width], cosine, sine).astype(jnp.bfloat16)
    v_ref[...] = projected[:, 2 * width :].astype(jnp.bfloat16)


def project(tokens, joined_w, cosine, sine):
    count, depth = tokens.shape
    width = joined_w.shape[1] // 3
    block = min(512, count)
    rows = lambda i: (i, 0)
    out = jax.ShapeDtypeStruct((count, width), jnp.bfloat16)
    return pl.pallas_call(
        qkv_kernel,
        grid=(count // block,),
        in_specs=[
            pl.BlockSpec((block, depth), rows),
            pl.BlockSpec((depth, 3 * width), lambda i: (0, 0), pipeline_mode=pl.Buffered(1)),
            pl.BlockSpec((block, cosine.shape[1]), rows),
            pl.BlockSpec((block, cosine.shape[1]), rows),
        ],
        out_specs=[pl.BlockSpec((block, width), rows)] * 3,
        out_shape=[out] * 3,
        compiler_params=pltpu.CompilerParams(vmem_limit_bytes=VMEM_MAX),
        name="qkv",
    )(tokens, joined_w, cosine, sine)


def head_parts(values):
    heads = values.shape[1] // HD
    if heads == 1:
        return [values]
    lane = lax.broadcasted_iota(jnp.int32, values.shape, 1) // HD
    return [jnp.where(lane == h, values, jnp.zeros_like(values)) for h in range(heads)]


def forward_kernel(bk, low_ref, q_ref, k_ref, v_ref, pos_ref, o_ref, lse_ref, vt, acc, top, total):
    row, i = pl.program_id(0), pl.program_id(1)
    bq, width = q_ref.shape
    heads = width // HD

    @pl.when(i == 0)
    def _():
        vt[...] = v_ref[...].T

    q_parts = head_parts(q_ref[...])
    q_index = i * bq + lax.broadcasted_iota(jnp.int32, (1, bq), 1)
    first = q_index - pos_ref[0]
    acc[...] = jnp.zeros_like(acc)
    top[...] = jnp.full_like(top, NEG)
    total[...] = jnp.zeros_like(total)

    def step(j, carry):
        at = pl.ds(pl.multiple_of(j * bk, bk), bk)
        keys = k_ref[at, :]
        k_index = j * bk + lax.broadcasted_iota(jnp.int32, (bk, bq), 0)
        allowed = (k_index >= first) & (k_index <= q_index)
        for h in range(heads):
            mine = slice(h * HD, (h + 1) * HD)
            scores = lax.dot_general(keys, q_parts[h], NT, preferred_element_type=jnp.float32)
            scores = jnp.where(allowed, scores, NEG)
            old = top[h : h + 1, :]
            new = jnp.maximum(old, jnp.max(scores, axis=0, keepdims=True))
            probs = jnp.exp(scores - new)
            fade = jnp.exp(old - new)
            top[h : h + 1, :] = new
            total[h : h + 1, :] = fade * total[h : h + 1, :] + jnp.sum(probs, axis=0, keepdims=True)
            acc[mine, :] = fade * acc[mine, :] + jnp.dot(
                vt[mine, at], probs.astype(jnp.bfloat16), preferred_element_type=jnp.float32
            )
        return carry

    lax.fori_loop(low_ref[row, i], ((i + 1) * bq + bk - 1) // bk, step, 0)
    for h in range(heads):
        mine = slice(h * HD, (h + 1) * HD)
        acc[mine, :] = acc[mine, :] / total[h : h + 1, :]
    o_ref[...] = acc[...].T.astype(jnp.bfloat16)
    lse_ref[0] = top[...] + jnp.log(jnp.maximum(total[...], 1e-30))


def attend_forward(q, k, v, positions, bq, bk):
    rows, length = positions.shape
    width = q.shape[1]
    per = length // bq
    starts = jnp.arange(0, length, bq, dtype=jnp.int32)
    low = (starts[None, :] - positions[:, ::bq]) // bk
    pos3 = positions[:, None, :]
    return pl.pallas_call(
        functools.partial(forward_kernel, bk),
        grid_spec=pltpu.PrefetchScalarGridSpec(
            num_scalar_prefetch=1,
            grid=(rows, per),
            in_specs=[
                pl.BlockSpec((bq, width), lambda r, i, low: (r * per + i, 0)),
                pl.BlockSpec((length, width), lambda r, i, low: (r, 0)),
                pl.BlockSpec((length, width), lambda r, i, low: (r, 0)),
                pl.BlockSpec((1, 1, bq), lambda r, i, low: (r, 0, i)),
            ],
            out_specs=[
                pl.BlockSpec((bq, width), lambda r, i, low: (r * per + i, 0)),
                pl.BlockSpec((1, 8, bq), lambda r, i, low: (r, 0, i)),
            ],
            scratch_shapes=[
                pltpu.VMEM((width, length), jnp.bfloat16),
                pltpu.VMEM((width, bq), jnp.float32),
                pltpu.VMEM((8, bq), jnp.float32),
                pltpu.VMEM((8, bq), jnp.float32),
            ],
        ),
        out_shape=[
            jax.ShapeDtypeStruct((rows * length, width), jnp.bfloat16),
            jax.ShapeDtypeStruct((rows, 8, length), jnp.float32),
        ],
        compiler_params=pltpu.CompilerParams(vmem_limit_bytes=VMEM_MAX),
        name="attend",
    )(low, q, k, v, pos3)


def backward_kernel(
    bk, bq, low_ref, q_ref, k_ref, v_ref, o_ref, do_ref, lse_ref, pos_ref, cos_ref, sin_ref, out_ref,
    kt, dqt, dk, dv,
):
    row, i = pl.program_id(0), pl.program_id(1)
    width = q_ref.shape[1]
    heads = width // HD
    here = pl.ds(pl.multiple_of(i * bq, bq), bq)

    @pl.when(i == 0)
    def _():
        kt[...] = k_ref[...].T
        dk[...] = jnp.zeros_like(dk)
        dv[...] = jnp.zeros_like(dv)

    grads = do_ref[here, :]
    q_parts = head_parts(q_ref[here, :])
    g_parts = head_parts(grads)
    stacked_q = jnp.concatenate(q_parts, axis=0)
    stacked_g = jnp.concatenate(g_parts, axis=0)
    products = grads.astype(jnp.float32) * o_ref[here, :].astype(jnp.float32)
    pick = (
        lax.broadcasted_iota(jnp.int32, (8, width), 1) // HD
        == lax.broadcasted_iota(jnp.int32, (8, width), 0)
    ).astype(jnp.float32)
    centre = lax.dot_general(
        pick, products, NT, precision=lax.Precision.HIGHEST, preferred_element_type=jnp.float32
    )
    level = lse_ref[0, :, here]
    q_index = i * bq + lax.broadcasted_iota(jnp.int32, (1, bq), 1)
    first = q_index - pos_ref[0, :, here]
    dqt[...] = jnp.zeros_like(dqt)

    def step(j, carry):
        at = pl.ds(pl.multiple_of(j * bk, bk), bk)
        keys, values = k_ref[at, :], v_ref[at, :]
        k_index = j * bk + lax.broadcasted_iota(jnp.int32, (bk, bq), 0)
        allowed = (k_index >= first) & (k_index <= q_index)
        all_p, all_s = [], []
        for h in range(heads):
            mine = slice(h * HD, (h + 1) * HD)
            scores = lax.dot_general(keys, q_parts[h], NT, preferred_element_type=jnp.float32)
            probs = jnp.where(allowed, jnp.exp(scores - level[h : h + 1, :]), 0.0)
            d_probs = lax.dot_general(values, g_parts[h], NT, preferred_element_type=jnp.float32)
            d_scores = (probs * (d_probs - centre[h : h + 1, :])).astype(jnp.bfloat16)
            dqt[mine, :] += jnp.dot(kt[mine, at], d_scores, preferred_element_type=jnp.float32)
            all_p.append(probs.astype(jnp.bfloat16))
            all_s.append(d_scores)
        dv[at, :] += jnp.dot(
            jnp.concatenate(all_p, axis=1), stacked_g, preferred_element_type=jnp.float32
        )
        dk[at, :] += jnp.dot(
            jnp.concatenate(all_s, axis=1), stacked_q, preferred_element_type=jnp.float32
        )
        return carry

    lax.fori_loop(low_ref[row, i], ((i + 1) * bq + bk - 1) // bk, step, 0)
    out_ref[here, 0:width] = turn_back(
        dqt[...].T * (HD**-0.5), cos_ref[here, :], sin_ref[here, :]
    ).astype(jnp.bfloat16)

    @pl.when(i == pl.num_programs(1) - 1)
    def _():
        out_ref[:, width : 2 * width] = turn_back(dk[...], cos_ref[...], sin_ref[...]).astype(
            jnp.bfloat16
        )
        out_ref[:, 2 * width : 3 * width] = dv[...].astype(jnp.bfloat16)


def attend_backward(q, k, v, o, d_o, lse, positions, cosine, sine, bq, bk):
    rows, length = positions.shape
    width = q.shape[1]
    per = length // bq
    starts = jnp.arange(0, length, bq, dtype=jnp.int32)
    low = (starts[None, :] - positions[:, ::bq]) // bk
    pos3 = positions[:, None, :]
    whole = pl.BlockSpec((length, width), lambda r, i, low: (r, 0))
    table = pl.BlockSpec((length, cosine.shape[1]), lambda r, i, low: (r, 0))
    return pl.pallas_call(
        functools.partial(backward_kernel, bk, bq),
        grid_spec=pltpu.PrefetchScalarGridSpec(
            num_scalar_prefetch=1,
            grid=(rows, per),
            in_specs=[whole] * 5
            + [
                pl.BlockSpec((1, 8, length), lambda r, i, low: (r, 0, 0)),
                pl.BlockSpec((1, 1, length), lambda r, i, low: (r, 0, 0)),
                table,
                table,
            ],
            out_specs=pl.BlockSpec((length, 3 * width), lambda r, i, low: (r, 0)),
            scratch_shapes=[
                pltpu.VMEM((width, length), jnp.bfloat16),
                pltpu.VMEM((width, bq), jnp.float32),
                pltpu.VMEM((length, width), jnp.float32),
                pltpu.VMEM((length, width), jnp.float32),
            ],
        ),
        out_shape=jax.ShapeDtypeStruct((rows * length, 3 * width), jnp.bfloat16),
        compiler_params=pltpu.CompilerParams(vmem_limit_bytes=VMEM_MAX),
        name="attend_back",
    )(low, q, k, v, o, d_o, lse, pos3, cosine, sine)


def mlp_kernel(n_ref, g_ref, wg_ref, wu_ref, wd_ref, hidden_ref, both_ref):
    ff = hidden_ref.shape[1]
    tokens = n_ref[...]
    gate = jnp.dot(tokens, wg_ref[...], preferred_element_type=jnp.float32)
    up = jnp.dot(tokens, wu_ref[...], preferred_element_type=jnp.float32)
    d_hidden = lax.dot_general(g_ref[...], wd_ref[...], NT, preferred_element_type=jnp.float32)
    sig = 1.0 / (1.0 + jnp.exp(-gate))
    act = gate * sig
    hidden_ref[...] = (act * up).astype(jnp.bfloat16)
    both_ref[:, ff:] = (d_hidden * act).astype(jnp.bfloat16)
    both_ref[:, :ff] = (d_hidden * up * (sig * (1.0 + gate * (1.0 - sig)))).astype(jnp.bfloat16)


def mlp_middle(tokens, grads, w_gate, w_up, w_down, block=256):
    count, depth = tokens.shape
    ff = w_gate.shape[1]
    block = min(block, count)
    rows = lambda i: (i, 0)
    fixed = lambda i: (0, 0)
    one = pl.Buffered(1)
    return pl.pallas_call(
        mlp_kernel,
        grid=(count // block,),
        in_specs=[
            pl.BlockSpec((block, depth), rows),
            pl.BlockSpec((block, depth), rows),
            pl.BlockSpec((depth, ff), fixed, pipeline_mode=one),
            pl.BlockSpec((depth, ff), fixed, pipeline_mode=one),
            pl.BlockSpec((ff, depth), fixed, pipeline_mode=one),
        ],
        out_specs=[pl.BlockSpec((block, ff), rows), pl.BlockSpec((block, 2 * ff), rows)],
        out_shape=[
            jax.ShapeDtypeStruct((count, ff), jnp.bfloat16),
            jax.ShapeDtypeStruct((count, 2 * ff), jnp.bfloat16),
        ],
        compiler_params=pltpu.CompilerParams(vmem_limit_bytes=VMEM_MAX),
        name="mlp_middle",
    )(tokens, grads, w_gate, w_up, w_down)


rope_theta = 130000.0
norm_eps = 1e-05


def rotary_tables(position_list, width):
    half_dim = HD // 2
    frequency = rope_theta ** (-(jnp.arange(half_dim, dtype=jnp.float32) * 2.0 / HD))
    angles = position_list.astype(jnp.float32)[:, None] * frequency[None, :]
    cosine, sine = jnp.cos(angles), jnp.sin(angles)
    times = width // HD
    return (
        jnp.concatenate([cosine, cosine] * times, axis=1),
        jnp.concatenate([-sine, sine] * times, axis=1),
    )


def normalize(row_values):
    inverse = lax.rsqrt(jnp.mean(row_values * row_values, axis=-1, keepdims=True) + norm_eps)
    return (row_values * inverse, inverse)


def norm_back(grad_in, gain_vec, unit_rows, inverse):
    scaled = grad_in * gain_vec
    return inverse * (scaled - unit_rows * jnp.mean(scaled * unit_rows, axis=-1, keepdims=True))


def sum_over_dp(pieces):
    if lax.axis_size("dp") != 4:
        return [lax.psum(piece, "dp") for piece in pieces]
    place = lax.axis_index("dp")
    inner = (place == 1) | (place == 2)
    sums = []
    for piece in pieces:
        arrived = lax.ppermute(piece, "dp", [(0, 1), (3, 2)])
        pair = piece + arrived
        arrived = lax.ppermute(pair, "dp", [(1, 2), (2, 1)])
        whole = pair + arrived
        arrived = lax.ppermute(whole, "dp", [(1, 0), (2, 3)])
        sums.append(jnp.where(inner, whole, arrived))
    return sums


def local(
    layer_input,
    gain_attn,
    w_query,
    w_key,
    w_value,
    w_out,
    gain_mlp,
    w_gate,
    w_up,
    w_down,
    segment_ids,
    positions,
    out_grad,
):
    width = layer_input.shape[1]
    hidden_w = w_query.shape[1]
    ff_local = w_gate.shape[1]
    length = positions.shape[1]
    bf16, f32 = jnp.bfloat16, jnp.float32
    block = min(512, length)
    gather = functools.partial(lax.all_gather, axis_name="tensor", axis=0, tiled=True)
    scatter = functools.partial(
        lax.psum_scatter, axis_name="tensor", scatter_dimension=0, tiled=True
    )
    joined_w = jnp.concatenate([w_query, w_key, w_value], axis=1)
    cosine, sine = rotary_tables(positions.reshape(-1), min(2 * HD, hidden_w))

    inputs = layer_input.astype(f32)
    unit_one, inverse_one = normalize(inputs)
    all_one = gather((unit_one * gain_attn).astype(bf16))
    all_w_out = gather(w_out)
    all_grad = gather(out_grad)
    queries, keys, values = project(all_one, joined_w, cosine, sine)
    attended, level = attend_forward(queries, keys, values, positions, block, block)
    mixed = lax.all_to_all(attended, "tensor", split_axis=0, concat_axis=1, tiled=True)
    residual = inputs + jnp.dot(mixed, all_w_out, preferred_element_type=f32)

    unit_two, inverse_two = normalize(residual)
    all_two = gather((unit_two * gain_mlp).astype(bf16))
    hidden, d_both = mlp_middle(all_two, all_grad, w_gate, w_up, w_down)
    dot_t = lambda a, b: lax.dot_general(
        a, b, (((0,), (0,)), ((), ())), preferred_element_type=f32
    ).astype(bf16)
    dot_n = lambda a, b: lax.dot_general(a, b, NT, preferred_element_type=f32)
    both_w = jnp.concatenate([w_gate, w_up], axis=1)
    d_two = scatter(dot_n(d_both, both_w).astype(bf16)).astype(f32)
    grad_down = dot_t(hidden, all_grad)
    grad_both = dot_t(all_two, d_both)
    layer_out = (
        residual + scatter(jnp.dot(hidden, w_down, preferred_element_type=f32).astype(bf16)).astype(f32)
    ).astype(bf16)

    gain_two_part = jnp.sum(d_two * unit_two, axis=0)
    d_residual = out_grad.astype(f32) + norm_back(d_two, gain_mlp, unit_two, inverse_two)
    d_attn = d_residual.astype(bf16)
    d_mixed = dot_n(d_attn, all_w_out).astype(bf16)
    d_attended = lax.all_to_all(d_mixed, "tensor", split_axis=1, concat_axis=0, tiled=True)
    grad_out = scatter(dot_t(mixed, d_attn))
    d_projected = attend_backward(
        queries, keys, values, attended, d_attended, level, positions, cosine, sine, block, block
    )
    d_one = scatter(dot_n(d_projected, joined_w).astype(bf16)).astype(f32)
    grad_joined = dot_t(all_one, d_projected)
    input_grad = d_residual + norm_back(d_one, gain_attn, unit_one, inverse_one)
    gain_one_part = (
        jnp.sum(grad_joined.astype(f32) * joined_w.astype(f32), axis=1) / gain_attn
    )

    half = grad_both.shape[0] // 2
    down, both_a, both_b, out, joined = sum_over_dp(
        [grad_down, grad_both[:half], grad_both[half:], grad_out, grad_joined]
    )
    both = jnp.concatenate([both_a, both_b], axis=0)
    gains = lax.psum(jnp.stack([gain_one_part, gain_two_part]), ("dp", "tensor"))
    gain_piece = width // lax.axis_size("tensor")
    gains = lax.dynamic_slice_in_dim(gains, lax.axis_index("tensor") * gain_piece, gain_piece, 1)
    return (
        layer_out,
        input_grad,
        gains[0],
        joined[:, :hidden_w].astype(f32),
        joined[:, hidden_w : 2 * hidden_w].astype(f32),
        joined[:, 2 * hidden_w :].astype(f32),
        out.astype(f32),
        gains[1],
        both[:, :ff_local].astype(f32),
        both[:, ff_local:].astype(f32),
        down.astype(f32),
    )


def solution(mesh):
    return jax.shard_map(
        local,
        mesh=mesh,
        in_specs=(
            P(("dp", "tensor"), None),
            P(),
            P(None, "tensor"),
            P(None, "tensor"),
            P(None, "tensor"),
            P("tensor", None),
            P(),
            P(None, "tensor"),
            P(None, "tensor"),
            P("tensor", None),
            P("dp", None),
            P("dp", None),
            P(("dp", "tensor"), None),
        ),
        out_specs=(
            P(("dp", "tensor"), None),
            P(("dp", "tensor"), None),
            P("tensor"),
            P(None, "tensor"),
            P(None, "tensor"),
            P(None, "tensor"),
            P("tensor", None),
            P("tensor"),
            P(None, "tensor"),
            P(None, "tensor"),
            P("tensor", None),
        ),
        check_vma=False,
    )
```

```python
import functools
import jax
import jax.numpy as jnp
from jax import lax
from jax.experimental import pallas as pl
from jax.experimental.pallas import tpu as pltpu
from jax.sharding import PartitionSpec as P


HD = 64
NEG = -1e30
NT = (((1,), (1,)), ((), ()))
VMEM_MAX = 60 * 1024 * 1024


def cost(flops, nbytes):
    return pl.CostEstimate(flops=flops, bytes_accessed=nbytes, transcendentals=0)


def swap_halves(values):
    width = values.shape[-1]
    if width == HD:
        return jnp.concatenate([values[:, HD // 2 :], values[:, : HD // 2]], axis=1)
    lane = lax.broadcasted_iota(jnp.int32, values.shape, 1)
    return jnp.where(
        lane % HD < HD // 2,
        pltpu.roll(values, width - HD // 2, 1),
        pltpu.roll(values, HD // 2, 1),
    )


def turn(values, cosine, sine):
    width = cosine.shape[-1]
    parts = []
    for start in range(0, values.shape[-1], width):
        piece = values[:, start : start + width]
        parts.append(piece * cosine + swap_halves(piece) * sine)
    return parts[0] if len(parts) == 1 else jnp.concatenate(parts, axis=1)


def turn_back(values, cosine, sine):
    width = cosine.shape[-1]
    parts = []
    for start in range(0, values.shape[-1], width):
        piece = values[:, start : start + width]
        parts.append(piece * cosine + swap_halves(piece * sine))
    return parts[0] if len(parts) == 1 else jnp.concatenate(parts, axis=1)


def qkv_kernel(x_ref, w_ref, cos_ref, sin_ref, q_ref, k_ref, v_ref):
    width = q_ref.shape[1]
    projected = jnp.dot(x_ref[...], w_ref[...], preferred_element_type=jnp.float32)
    cosine, sine = cos_ref[...], sin_ref[...]
    turned = turn(projected[:, :width], cosine, sine).astype(jnp.bfloat16)
    q_ref[...] = turned * jnp.bfloat16(HD**-0.5)
    k_ref[...] = turn(projected[:, width : 2 * width], cosine, sine).astype(jnp.bfloat16)
    v_ref[...] = projected[:, 2 * width :].astype(jnp.bfloat16)


def project(tokens, joined_w, cosine, sine):
    count, depth = tokens.shape
    width = joined_w.shape[1] // 3
    block = min(512, count)
    rows = lambda i: (i, 0)
    out = jax.ShapeDtypeStruct((count, width), jnp.bfloat16)
    return pl.pallas_call(
        qkv_kernel,
        grid=(count // block,),
        in_specs=[
            pl.BlockSpec((block, depth), rows),
            pl.BlockSpec((depth, 3 * width), lambda i: (0, 0), pipeline_mode=pl.Buffered(1)),
            pl.BlockSpec((block, cosine.shape[1]), rows),
            pl.BlockSpec((block, cosine.shape[1]), rows),
        ],
        out_specs=[pl.BlockSpec((block, width), rows)] * 3,
        out_shape=[out] * 3,
        compiler_params=pltpu.CompilerParams(vmem_limit_bytes=VMEM_MAX),
        cost_estimate=cost(6 * count * depth * width, 2 * count * depth),
        name="qkv",
    )(tokens, joined_w, cosine, sine)


def head_parts(values):
    heads = values.shape[1] // HD
    if heads == 1:
        return [values]
    lane = lax.broadcasted_iota(jnp.int32, values.shape, 1) // HD
    return [jnp.where(lane == h, values, jnp.zeros_like(values)) for h in range(heads)]


def forward_kernel(bk, low_ref, q_ref, k_ref, v_ref, pos_ref, o_ref, lse_ref, vt, acc, top, total):
    row, i = pl.program_id(0), pl.program_id(1)
    bq, width = q_ref.shape
    heads = width // HD

    @pl.when(i == 0)
    def _():
        vt[...] = v_ref[...].T

    q_parts = head_parts(q_ref[...])
    q_index = i * bq + lax.broadcasted_iota(jnp.int32, (1, bq), 1)
    first = q_index - pos_ref[0]
    acc[...] = jnp.zeros_like(acc)
    top[...] = jnp.full_like(top, NEG)
    total[...] = jnp.zeros_like(total)

    def step(j, carry):
        at = pl.ds(pl.multiple_of(j * bk, bk), bk)
        keys = k_ref[at, :]
        k_index = j * bk + lax.broadcasted_iota(jnp.int32, (bk, bq), 0)
        allowed = (k_index >= first) & (k_index <= q_index)
        for h in range(heads):
            mine = slice(h * HD, (h + 1) * HD)
            scores = lax.dot_general(keys, q_parts[h], NT, preferred_element_type=jnp.float32)
            scores = jnp.where(allowed, scores, NEG)
            old = top[h : h + 1, :]
            new = jnp.maximum(old, jnp.max(scores, axis=0, keepdims=True))
            probs = jnp.exp(scores - new)
            fade = jnp.exp(old - new)
            top[h : h + 1, :] = new
            total[h : h + 1, :] = fade * total[h : h + 1, :] + jnp.sum(probs, axis=0, keepdims=True)
            acc[mine, :] = fade * acc[mine, :] + jnp.dot(
                vt[mine, at], probs.astype(jnp.bfloat16), preferred_element_type=jnp.float32
            )
        return carry

    lax.fori_loop(low_ref[row, i], ((i + 1) * bq + bk - 1) // bk, step, 0)
    for h in range(heads):
        mine = slice(h * HD, (h + 1) * HD)
        acc[mine, :] = acc[mine, :] / total[h : h + 1, :]
    o_ref[...] = acc[...].T.astype(jnp.bfloat16)
    lse_ref[0] = top[...] + jnp.log(jnp.maximum(total[...], 1e-30))


def attend_forward(q, k, v, positions, bq, bk):
    rows, length = positions.shape
    width = q.shape[1]
    per = length // bq
    starts = jnp.arange(0, length, bq, dtype=jnp.int32)
    low = (starts[None, :] - positions[:, ::bq]) // bk
    pos3 = positions[:, None, :]
    return pl.pallas_call(
        functools.partial(forward_kernel, bk),
        grid_spec=pltpu.PrefetchScalarGridSpec(
            num_scalar_prefetch=1,
            grid=(rows, per),
            in_specs=[
                pl.BlockSpec((bq, width), lambda r, i, low: (r * per + i, 0)),
                pl.BlockSpec((length, width), lambda r, i, low: (r, 0)),
                pl.BlockSpec((length, width), lambda r, i, low: (r, 0)),
                pl.BlockSpec((1, 1, bq), lambda r, i, low: (r, 0, i)),
            ],
            out_specs=[
                pl.BlockSpec((bq, width), lambda r, i, low: (r * per + i, 0)),
                pl.BlockSpec((1, 8, bq), lambda r, i, low: (r, 0, i)),
            ],
            scratch_shapes=[
                pltpu.VMEM((width, length), jnp.bfloat16),
                pltpu.VMEM((width, bq), jnp.float32),
                pltpu.VMEM((8, bq), jnp.float32),
                pltpu.VMEM((8, bq), jnp.float32),
            ],
        ),
        out_shape=[
            jax.ShapeDtypeStruct((rows * length, width), jnp.bfloat16),
            jax.ShapeDtypeStruct((rows, 8, length), jnp.float32),
        ],
        compiler_params=pltpu.CompilerParams(vmem_limit_bytes=VMEM_MAX),
        cost_estimate=cost(16 * rows * length * length * width, 10 * rows * length * width),
        name="attend",
    )(low, q, k, v, pos3)


def backward_kernel(
    bk, bq, low_ref, q_ref, k_ref, v_ref, o_ref, do_ref, lse_ref, pos_ref, cos_ref, sin_ref, out_ref,
    kt, dqt, dk, dv,
):
    row, i = pl.program_id(0), pl.program_id(1)
    width = q_ref.shape[1]
    heads = width // HD
    here = pl.ds(pl.multiple_of(i * bq, bq), bq)

    @pl.when(i == 0)
    def _():
        kt[...] = k_ref[...].T
        dk[...] = jnp.zeros_like(dk)
        dv[...] = jnp.zeros_like(dv)

    grads = do_ref[here, :]
    q_parts = head_parts(q_ref[here, :])
    g_parts = head_parts(grads)
    stacked_q = jnp.concatenate(q_parts, axis=0)
    stacked_g = jnp.concatenate(g_parts, axis=0)
    products = grads.astype(jnp.float32) * o_ref[here, :].astype(jnp.float32)
    pick = (
        lax.broadcasted_iota(jnp.int32, (8, width), 1) // HD
        == lax.broadcasted_iota(jnp.int32, (8, width), 0)
    ).astype(jnp.float32)
    centre = lax.dot_general(
        pick, products, NT, precision=lax.Precision.HIGHEST, preferred_element_type=jnp.float32
    )
    level = lse_ref[0, :, here]
    q_index = i * bq + lax.broadcasted_iota(jnp.int32, (1, bq), 1)
    first = q_index - pos_ref[0, :, here]
    dqt[...] = jnp.zeros_like(dqt)

    def step(j, carry):
        at = pl.ds(pl.multiple_of(j * bk, bk), bk)
        keys, values = k_ref[at, :], v_ref[at, :]
        k_index = j * bk + lax.broadcasted_iota(jnp.int32, (bk, bq), 0)
        allowed = (k_index >= first) & (k_index <= q_index)
        all_p, all_s = [], []
        for h in range(heads):
            mine = slice(h * HD, (h + 1) * HD)
            scores = lax.dot_general(keys, q_parts[h], NT, preferred_element_type=jnp.float32)
            probs = jnp.where(allowed, jnp.exp(scores - level[h : h + 1, :]), 0.0)
            d_probs = lax.dot_general(values, g_parts[h], NT, preferred_element_type=jnp.float32)
            d_scores = (probs * (d_probs - centre[h : h + 1, :])).astype(jnp.bfloat16)
            dqt[mine, :] += jnp.dot(kt[mine, at], d_scores, preferred_element_type=jnp.float32)
            all_p.append(probs.astype(jnp.bfloat16))
            all_s.append(d_scores)
        dv[at, :] += jnp.dot(
            jnp.concatenate(all_p, axis=1), stacked_g, preferred_element_type=jnp.float32
        )
        dk[at, :] += jnp.dot(
            jnp.concatenate(all_s, axis=1), stacked_q, preferred_element_type=jnp.float32
        )
        return carry

    lax.fori_loop(low_ref[row, i], ((i + 1) * bq + bk - 1) // bk, step, 0)
    out_ref[here, 0:width] = turn_back(
        dqt[...].T * (HD**-0.5), cos_ref[here, :], sin_ref[here, :]
    ).astype(jnp.bfloat16)

    @pl.when(i == pl.num_programs(1) - 1)
    def _():
        out_ref[:, width : 2 * width] = turn_back(dk[...], cos_ref[...], sin_ref[...]).astype(
            jnp.bfloat16
        )
        out_ref[:, 2 * width : 3 * width] = dv[...].astype(jnp.bfloat16)


def attend_backward(row, so_far, q, k, v, o, d_o, lse, positions, cosine, sine, bq, bk):
    rows, length = positions.shape
    width = q.shape[1]
    per = length // bq
    starts = jnp.arange(0, length, bq, dtype=jnp.int32)
    low = (starts[None, :] - positions[row : row + 1, ::bq]) // bk
    pos3 = positions[:, None, :]
    whole = pl.BlockSpec((length, width), lambda r, i, low: (row, 0))
    table = pl.BlockSpec((length, cosine.shape[1]), lambda r, i, low: (row, 0))
    arrays = [low, q, k, v, o, d_o, lse, pos3, cosine, sine]
    specs = [whole] * 5 + [
        pl.BlockSpec((1, 8, length), lambda r, i, low: (row, 0, 0)),
        pl.BlockSpec((1, 1, length), lambda r, i, low: (row, 0, 0)),
        table,
        table,
    ]
    body, alias = functools.partial(backward_kernel, bk, bq), {}
    if so_far is not None:
        arrays.append(so_far)
        specs.append(pl.BlockSpec(memory_space=pl.ANY))
        alias = {len(arrays) - 1: 0}
        body = lambda *refs: backward_kernel(bk, bq, *refs[:10], *refs[11:])
    return pl.pallas_call(
        body,
        grid_spec=pltpu.PrefetchScalarGridSpec(
            num_scalar_prefetch=1,
            grid=(1, per),
            in_specs=specs,
            out_specs=pl.BlockSpec((length, 3 * width), lambda r, i, low: (row, 0)),
            scratch_shapes=[
                pltpu.VMEM((width, length), jnp.bfloat16),
                pltpu.VMEM((width, bq), jnp.float32),
                pltpu.VMEM((length, width), jnp.float32),
                pltpu.VMEM((length, width), jnp.float32),
            ],
        ),
        out_shape=jax.ShapeDtypeStruct((rows * length, 3 * width), jnp.bfloat16),
        input_output_aliases=alias,
        compiler_params=pltpu.CompilerParams(vmem_limit_bytes=VMEM_MAX),
        cost_estimate=cost(28 * length * length * width, 20 * length * width),
        name="attend_back",
    )(*arrays)


def mlp_kernel(n_ref, g_ref, wg_ref, wu_ref, wd_ref, hidden_ref, both_ref):
    ff = hidden_ref.shape[1]
    tokens = n_ref[...]
    gate = jnp.dot(tokens, wg_ref[...], preferred_element_type=jnp.float32)
    up = jnp.dot(tokens, wu_ref[...], preferred_element_type=jnp.float32)
    d_hidden = lax.dot_general(g_ref[...], wd_ref[...], NT, preferred_element_type=jnp.float32)
    sig = 1.0 / (1.0 + jnp.exp(-gate))
    act = gate * sig
    hidden_ref[...] = (act * up).astype(jnp.bfloat16)
    both_ref[:, ff:] = (d_hidden * act).astype(jnp.bfloat16)
    both_ref[:, :ff] = (d_hidden * up * (sig * (1.0 + gate * (1.0 - sig)))).astype(jnp.bfloat16)


def mlp_middle(tokens, grads, w_gate, w_up, w_down, block=256):
    count, depth = tokens.shape
    ff = w_gate.shape[1]
    block = min(block, count)
    rows = lambda i: (i, 0)
    fixed = lambda i: (0, 0)
    one = pl.Buffered(1)
    return pl.pallas_call(
        mlp_kernel,
        grid=(count // block,),
        in_specs=[
            pl.BlockSpec((block, depth), rows),
            pl.BlockSpec((block, depth), rows),
            pl.BlockSpec((depth, ff), fixed, pipeline_mode=one),
            pl.BlockSpec((depth, ff), fixed, pipeline_mode=one),
            pl.BlockSpec((ff, depth), fixed, pipeline_mode=one),
        ],
        out_specs=[pl.BlockSpec((block, ff), rows), pl.BlockSpec((block, 2 * ff), rows)],
        out_shape=[
            jax.ShapeDtypeStruct((count, ff), jnp.bfloat16),
            jax.ShapeDtypeStruct((count, 2 * ff), jnp.bfloat16),
        ],
        compiler_params=pltpu.CompilerParams(vmem_limit_bytes=VMEM_MAX),
        cost_estimate=cost(6 * count * depth * ff, 4 * count * depth),
        name="mlp_middle",
    )(tokens, grads, w_gate, w_up, w_down)


rope_theta = 130000.0
norm_eps = 1e-05


def rotary_tables(position_list, width):
    half_dim = HD // 2
    frequency = rope_theta ** (-(jnp.arange(half_dim, dtype=jnp.float32) * 2.0 / HD))
    angles = position_list.astype(jnp.float32)[:, None] * frequency[None, :]
    cosine, sine = jnp.cos(angles), jnp.sin(angles)
    times = width // HD
    return (
        jnp.concatenate([cosine, cosine] * times, axis=1),
        jnp.concatenate([-sine, sine] * times, axis=1),
    )


def normalize(row_values):
    inverse = lax.rsqrt(jnp.mean(row_values * row_values, axis=-1, keepdims=True) + norm_eps)
    return (row_values * inverse, inverse)


def norm_back(grad_in, gain_vec, unit_rows, inverse):
    scaled = grad_in * gain_vec
    return inverse * (scaled - unit_rows * jnp.mean(scaled * unit_rows, axis=-1, keepdims=True))


def hop(piece, moves):
    return lax.ppermute(piece, "dp", moves)


def sum_over_dp(piece):
    if lax.axis_size("dp") != 4:
        return lax.psum(piece, "dp").astype(jnp.float32)
    place = lax.axis_index("dp")
    inner = (place == 1) | (place == 2)
    pair = piece + hop(piece, [(0, 1), (3, 2)])
    whole = pair + hop(pair, [(1, 2), (2, 1)])
    arrived = hop(whole, [(1, 0), (2, 3)])
    return jnp.where(inner, whole, arrived).astype(jnp.float32)


def local(
    layer_input,
    gain_attn,
    w_query,
    w_key,
    w_value,
    w_out,
    gain_mlp,
    w_gate,
    w_up,
    w_down,
    segment_ids,
    positions,
    out_grad,
):
    width = layer_input.shape[1]
    hidden_w = w_query.shape[1]
    ff_local = w_gate.shape[1]
    length = positions.shape[1]
    bf16, f32 = jnp.bfloat16, jnp.float32
    block = min(512, length)

    def gather(value):
        return lax.all_gather(value, "tensor", axis=0, tiled=True)

    def scatter(value):
        return lax.psum_scatter(value, "tensor", scatter_dimension=0, tiled=True)

    def mm(a, b, dims=(((1,), (0,)), ((), ()))):
        return lax.dot_general(a, b, dims, preferred_element_type=f32)

    TN = (((0,), (0,)), ((), ()))
    joined_w = jnp.concatenate([w_query, w_key, w_value], axis=1)
    both_w = jnp.concatenate([w_gate, w_up], axis=1)
    cosine, sine = rotary_tables(positions.reshape(-1), min(2 * HD, hidden_w))

    inputs = layer_input.astype(f32)
    unit_one, inverse_one = normalize(inputs)
    all_one = gather((unit_one * gain_attn).astype(bf16))
    all_grad = gather(out_grad)
    all_w_out = gather(w_out)
    queries, keys, values = project(all_one, joined_w, cosine, sine)
    attended, level = attend_forward(queries, keys, values, positions, block, block)
    mixed = lax.all_to_all(attended, "tensor", split_axis=0, concat_axis=1, tiled=True)
    residual = inputs + mm(mixed, all_w_out)

    unit_two, inverse_two = normalize(residual)
    all_two = gather((unit_two * gain_mlp).astype(bf16))
    hidden, d_both = mlp_middle(all_two, all_grad, w_gate, w_up, w_down)
    grad_down = mm(hidden, all_grad, TN).astype(bf16)
    d_two = scatter(mm(d_both, both_w, NT).astype(bf16)).astype(f32)
    grad_gate = mm(all_two, d_both[:, :ff_local], TN).astype(bf16)
    grad_up = mm(all_two, d_both[:, ff_local:], TN).astype(bf16)
    layer_sum = scatter(mm(hidden, w_down).astype(bf16))

    gain_two_part = jnp.sum(d_two * unit_two, axis=0)
    d_residual = out_grad.astype(f32) + norm_back(d_two, gain_mlp, unit_two, inverse_two)
    d_attn = d_residual.astype(bf16)
    d_mixed = mm(d_attn, all_w_out, NT).astype(bf16)
    d_attended = lax.all_to_all(d_mixed, "tensor", split_axis=1, concat_axis=0, tiled=True)
    grad_out = scatter(mm(mixed, d_attn, TN).astype(bf16))
    d_projected = None
    for row in range(positions.shape[0]):
        d_projected = attend_backward(
            row, d_projected, queries, keys, values, attended, d_attended, level, positions,
            cosine, sine, block, block,
        )
    layer_sum, d_projected = lax.optimization_barrier((layer_sum, d_projected))
    layer_out = (residual + layer_sum.astype(f32)).astype(bf16)
    d_one = scatter(mm(d_projected, joined_w, NT).astype(bf16)).astype(f32)
    grad_joined = mm(all_one, d_projected, TN).astype(bf16)
    plain_joined = lax.optimization_barrier(grad_joined)
    gain_one_part = jnp.sum(plain_joined.astype(f32) * joined_w.astype(f32), axis=1) / gain_attn
    gains = lax.psum_scatter(
        jnp.stack([gain_one_part, gain_two_part]), "tensor", scatter_dimension=1, tiled=True
    )
    gains = sum_over_dp(gains)
    input_grad = d_residual + norm_back(d_one, gain_attn, unit_one, inverse_one)

    down = sum_over_dp(grad_down)
    gate = sum_over_dp(grad_gate)
    up = sum_over_dp(grad_up)
    rest = jnp.concatenate([grad_joined, grad_out.reshape(width, hidden_w)], axis=1)
    middle = width // 2
    rest = jnp.concatenate([sum_over_dp(rest[:middle]), sum_over_dp(rest[middle:])], axis=0)
    return (
        layer_out,
        input_grad,
        gains[0],
        rest[:, :hidden_w],
        rest[:, hidden_w : 2 * hidden_w],
        rest[:, 2 * hidden_w : 3 * hidden_w],
        rest[:, 3 * hidden_w :].reshape(hidden_w, width),
        gains[1],
        gate,
        up,
        down,
    )


def solution(mesh):
    return jax.shard_map(
        local,
        mesh=mesh,
        in_specs=(
            P(("dp", "tensor"), None),
            P(),
            P(None, "tensor"),
            P(None, "tensor"),
            P(None, "tensor"),
            P("tensor", None),
            P(),
            P(None, "tensor"),
            P(None, "tensor"),
            P("tensor", None),
            P("dp", None),
            P("dp", None),
            P(("dp", "tensor"), None),
        ),
        out_specs=(
            P(("dp", "tensor"), None),
            P(("dp", "tensor"), None),
            P("tensor"),
            P(None, "tensor"),
            P(None, "tensor"),
            P(None, "tensor"),
            P("tensor", None),
            P("tensor"),
            P(None, "tensor"),
            P(None, "tensor"),
            P("tensor", None),
        ),
        check_vma=False,
    )
```

```python
import functools
import jax
import jax.numpy as jnp
from jax import lax
from jax.experimental import pallas as pl
from jax.experimental.pallas import tpu as pltpu
from jax.sharding import PartitionSpec as P


HD = 64
NEG = -1e30
NT = (((1,), (1,)), ((), ()))
VMEM_MAX = 60 * 1024 * 1024


def cost(flops, nbytes):
    return pl.CostEstimate(flops=flops, bytes_accessed=nbytes, transcendentals=0)


def swap_halves(values):
    width = values.shape[-1]
    if width == HD:
        return jnp.concatenate([values[:, HD // 2 :], values[:, : HD // 2]], axis=1)
    lane = lax.broadcasted_iota(jnp.int32, values.shape, 1)
    return jnp.where(
        lane % HD < HD // 2,
        pltpu.roll(values, width - HD // 2, 1),
        pltpu.roll(values, HD // 2, 1),
    )


def turn(values, cosine, sine):
    return values * cosine + swap_halves(values) * sine


def turn_back(values, cosine, sine):
    return values * cosine + swap_halves(values * sine)


def group_width(width):
    return min(2 * HD, width)


def qkv_kernel(x_ref, w_ref, cos_ref, sin_ref, q_ref, k_ref, v_ref):
    size = group_width(q_ref.shape[1])
    projected = jnp.dot(x_ref[...], w_ref[...], preferred_element_type=jnp.float32)
    cosine, sine = cos_ref[...], sin_ref[...]
    for start in range(0, q_ref.shape[1], size):
        part = lambda n: projected[:, 3 * start + n * size : 3 * start + (n + 1) * size]
        mine = slice(start, start + size)
        turned = turn(part(0), cosine, sine).astype(jnp.bfloat16)
        q_ref[:, mine] = turned * jnp.bfloat16(HD**-0.5)
        k_ref[:, mine] = turn(part(1), cosine, sine).astype(jnp.bfloat16)
        v_ref[:, mine] = part(2).astype(jnp.bfloat16)


def project(tokens, joined_w, cosine, sine):
    count, depth = tokens.shape
    width = joined_w.shape[1] // 3
    block = min(512, count)
    rows = lambda i: (i, 0)
    out = jax.ShapeDtypeStruct((count, width), jnp.bfloat16)
    return pl.pallas_call(
        qkv_kernel,
        grid=(count // block,),
        in_specs=[
            pl.BlockSpec((block, depth), rows),
            pl.BlockSpec((depth, 3 * width), lambda i: (0, 0), pipeline_mode=pl.Buffered(1)),
            pl.BlockSpec((block, cosine.shape[1]), rows),
            pl.BlockSpec((block, cosine.shape[1]), rows),
        ],
        out_specs=[pl.BlockSpec((block, width), rows)] * 3,
        out_shape=[out] * 3,
        compiler_params=pltpu.CompilerParams(vmem_limit_bytes=VMEM_MAX),
        cost_estimate=cost(6 * count * depth * width, 2 * count * depth),
        name="qkv",
    )(tokens, joined_w, cosine, sine)


def head_parts(values):
    heads = values.shape[1] // HD
    if heads == 1:
        return [values]
    lane = lax.broadcasted_iota(jnp.int32, values.shape, 1) // HD
    return [jnp.where(lane == h, values, jnp.zeros_like(values)) for h in range(heads)]


def forward_kernel(bk, low_ref, q_ref, k_ref, v_ref, pos_ref, o_ref, lse_ref, vt, acc, top, total):
    row, i = pl.program_id(0), pl.program_id(1)
    bq, width = q_ref.shape
    heads = width // HD

    @pl.when(i == 0)
    def _():
        vt[...] = v_ref[...].T

    q_parts = head_parts(q_ref[...])
    q_index = i * bq + lax.broadcasted_iota(jnp.int32, (1, bq), 1)
    first = q_index - pos_ref[0]
    acc[...] = jnp.zeros_like(acc)
    top[...] = jnp.full_like(top, NEG)
    total[...] = jnp.zeros_like(total)

    def step(j, carry):
        at = pl.ds(pl.multiple_of(j * bk, bk), bk)
        keys = k_ref[at, :]
        k_index = j * bk + lax.broadcasted_iota(jnp.int32, (bk, bq), 0)
        allowed = (k_index >= first) & (k_index <= q_index)
        for h in range(heads):
            mine = slice(h * HD, (h + 1) * HD)
            scores = lax.dot_general(keys, q_parts[h], NT, preferred_element_type=jnp.float32)
            scores = jnp.where(allowed, scores, NEG)
            old = top[h : h + 1, :]
            new = jnp.maximum(old, jnp.max(scores, axis=0, keepdims=True))
            probs = jnp.exp(scores - new)
            fade = jnp.exp(old - new)
            top[h : h + 1, :] = new
            total[h : h + 1, :] = fade * total[h : h + 1, :] + jnp.sum(probs, axis=0, keepdims=True)
            acc[mine, :] = fade * acc[mine, :] + jnp.dot(
                vt[mine, at], probs.astype(jnp.bfloat16), preferred_element_type=jnp.float32
            )
        return carry

    lax.fori_loop(low_ref[row, i], ((i + 1) * bq + bk - 1) // bk, step, 0)
    for h in range(heads):
        mine = slice(h * HD, (h + 1) * HD)
        acc[mine, :] = acc[mine, :] / total[h : h + 1, :]
    o_ref[...] = acc[...].T.astype(jnp.bfloat16)
    lse_ref[0] = top[...] + jnp.log(jnp.maximum(total[...], 1e-30))


def attend_forward(q, k, v, positions, bq, bk):
    rows, length = positions.shape
    width = q.shape[1]
    per = length // bq
    starts = jnp.arange(0, length, bq, dtype=jnp.int32)
    low = (starts[None, :] - positions[:, ::bq]) // bk
    pos3 = positions[:, None, :]
    return pl.pallas_call(
        functools.partial(forward_kernel, bk),
        grid_spec=pltpu.PrefetchScalarGridSpec(
            num_scalar_prefetch=1,
            grid=(rows, per),
            in_specs=[
                pl.BlockSpec((bq, width), lambda r, i, low: (r * per + i, 0)),
                pl.BlockSpec((length, width), lambda r, i, low: (r, 0)),
                pl.BlockSpec((length, width), lambda r, i, low: (r, 0)),
                pl.BlockSpec((1, 1, bq), lambda r, i, low: (r, 0, i)),
            ],
            out_specs=[
                pl.BlockSpec((bq, width), lambda r, i, low: (r * per + i, 0)),
                pl.BlockSpec((1, 8, bq), lambda r, i, low: (r, 0, i)),
            ],
            scratch_shapes=[
                pltpu.VMEM((width, length), jnp.bfloat16),
                pltpu.VMEM((width, bq), jnp.float32),
                pltpu.VMEM((8, bq), jnp.float32),
                pltpu.VMEM((8, bq), jnp.float32),
            ],
        ),
        out_shape=[
            jax.ShapeDtypeStruct((rows * length, width), jnp.bfloat16),
            jax.ShapeDtypeStruct((rows, 8, length), jnp.float32),
        ],
        compiler_params=pltpu.CompilerParams(vmem_limit_bytes=VMEM_MAX),
        cost_estimate=cost(16 * rows * length * length * width, 10 * rows * length * width),
        name="attend",
    )(low, q, k, v, pos3)


def backward_kernel(
    first_head, bk, bq, low_ref, q_ref, k_ref, v_ref, o_ref, do_ref, lse_ref, pos_ref, cos_ref, sin_ref, out_ref,
    kt, dqt, dk, dv,
):
    row, i = pl.program_id(0), pl.program_id(1)
    width = q_ref.shape[1]
    heads = width // HD
    here = pl.ds(pl.multiple_of(i * bq, bq), bq)

    @pl.when(i == 0)
    def _():
        kt[...] = k_ref[...].T
        dk[...] = jnp.zeros_like(dk)
        dv[...] = jnp.zeros_like(dv)

    grads = do_ref[here, :]
    q_parts = head_parts(q_ref[here, :])
    g_parts = head_parts(grads)
    stacked_q = jnp.concatenate(q_parts, axis=0)
    stacked_g = jnp.concatenate(g_parts, axis=0)
    products = grads.astype(jnp.float32) * o_ref[here, :].astype(jnp.float32)
    pick = (
        lax.broadcasted_iota(jnp.int32, (8, width), 1) // HD
        == lax.broadcasted_iota(jnp.int32, (8, width), 0)
    ).astype(jnp.float32)
    centre = lax.dot_general(
        pick, products, NT, precision=lax.Precision.HIGHEST, preferred_element_type=jnp.float32
    )
    level = lse_ref[0, first_head : first_head + heads, here]
    q_index = i * bq + lax.broadcasted_iota(jnp.int32, (1, bq), 1)
    first = q_index - pos_ref[0, :, here]
    dqt[...] = jnp.zeros_like(dqt)

    def step(j, carry):
        at = pl.ds(pl.multiple_of(j * bk, bk), bk)
        keys, values = k_ref[at, :], v_ref[at, :]
        k_index = j * bk + lax.broadcasted_iota(jnp.int32, (bk, bq), 0)
        allowed = (k_index >= first) & (k_index <= q_index)
        all_p, all_s = [], []
        for h in range(heads):
            mine = slice(h * HD, (h + 1) * HD)
            scores = lax.dot_general(keys, q_parts[h], NT, preferred_element_type=jnp.float32)
            probs = jnp.where(allowed, jnp.exp(scores - level[h : h + 1, :]), 0.0)
            d_probs = lax.dot_general(values, g_parts[h], NT, preferred_element_type=jnp.float32)
            d_scores = (probs * (d_probs - centre[h : h + 1, :])).astype(jnp.bfloat16)
            dqt[mine, :] += jnp.dot(kt[mine, at], d_scores, preferred_element_type=jnp.float32)
            all_p.append(probs.astype(jnp.bfloat16))
            all_s.append(d_scores)
        dv[at, :] += jnp.dot(
            jnp.concatenate(all_p, axis=1), stacked_g, preferred_element_type=jnp.float32
        )
        dk[at, :] += jnp.dot(
            jnp.concatenate(all_s, axis=1), stacked_q, preferred_element_type=jnp.float32
        )
        return carry

    lax.fori_loop(low_ref[row, i], ((i + 1) * bq + bk - 1) // bk, step, 0)
    out_ref[here, 0:width] = turn_back(
        dqt[...].T * (HD**-0.5), cos_ref[here, :], sin_ref[here, :]
    ).astype(jnp.bfloat16)

    @pl.when(i == pl.num_programs(1) - 1)
    def _():
        out_ref[:, width : 2 * width] = turn_back(dk[...], cos_ref[...], sin_ref[...]).astype(
            jnp.bfloat16
        )
        out_ref[:, 2 * width : 3 * width] = dv[...].astype(jnp.bfloat16)


def attend_backward(group, q, k, v, o, d_o, lse, positions, cosine, sine, bq, bk):
    rows, length = positions.shape
    width = group_width(q.shape[1])
    per = length // bq
    starts = jnp.arange(0, length, bq, dtype=jnp.int32)
    low = (starts[None, :] - positions[:, ::bq]) // bk
    pos3 = positions[:, None, :]
    whole = pl.BlockSpec((length, width), lambda r, i, low: (r, group))
    table = pl.BlockSpec((length, width), lambda r, i, low: (r, 0))
    return pl.pallas_call(
        functools.partial(backward_kernel, group * (width // HD), bk, bq),
        grid_spec=pltpu.PrefetchScalarGridSpec(
            num_scalar_prefetch=1,
            grid=(rows, per),
            in_specs=[whole] * 5
            + [
                pl.BlockSpec((1, 8, length), lambda r, i, low: (r, 0, 0)),
                pl.BlockSpec((1, 1, length), lambda r, i, low: (r, 0, 0)),
                table,
                table,
            ],
            out_specs=pl.BlockSpec((length, 3 * width), lambda r, i, low: (r, 0)),
            scratch_shapes=[
                pltpu.VMEM((width, length), jnp.bfloat16),
                pltpu.VMEM((width, bq), jnp.float32),
                pltpu.VMEM((length, width), jnp.float32),
                pltpu.VMEM((length, width), jnp.float32),
            ],
        ),
        out_shape=jax.ShapeDtypeStruct((rows * length, 3 * width), jnp.bfloat16),
        compiler_params=pltpu.CompilerParams(vmem_limit_bytes=VMEM_MAX),
        cost_estimate=cost(28 * rows * length * length * width, 20 * rows * length * width),
        name="attend_back",
    )(low, q, k, v, o, d_o, lse, pos3, cosine, sine)


def mlp_kernel(n_ref, g_ref, wg_ref, wu_ref, wd_ref, hidden_ref, both_ref):
    ff = hidden_ref.shape[1]
    tokens = n_ref[...]
    gate = jnp.dot(tokens, wg_ref[...], preferred_element_type=jnp.float32)
    up = jnp.dot(tokens, wu_ref[...], preferred_element_type=jnp.float32)
    d_hidden = lax.dot_general(g_ref[...], wd_ref[...], NT, preferred_element_type=jnp.float32)
    sig = 1.0 / (1.0 + jnp.exp(-gate))
    act = gate * sig
    hidden_ref[...] = (act * up).astype(jnp.bfloat16)
    both_ref[:, ff:] = (d_hidden * act).astype(jnp.bfloat16)
    both_ref[:, :ff] = (d_hidden * up * (sig * (1.0 + gate * (1.0 - sig)))).astype(jnp.bfloat16)


def mlp_middle(tokens, grads, w_gate, w_up, w_down, block=256):
    count, depth = tokens.shape
    ff = w_gate.shape[1]
    block = min(block, count)
    rows = lambda i: (i, 0)
    fixed = lambda i: (0, 0)
    one = pl.Buffered(1)
    return pl.pallas_call(
        mlp_kernel,
        grid=(count // block,),
        in_specs=[
            pl.BlockSpec((block, depth), rows),
            pl.BlockSpec((block, depth), rows),
            pl.BlockSpec((depth, ff), fixed, pipeline_mode=one),
            pl.BlockSpec((depth, ff), fixed, pipeline_mode=one),
            pl.BlockSpec((ff, depth), fixed, pipeline_mode=one),
        ],
        out_specs=[pl.BlockSpec((block, ff), rows), pl.BlockSpec((block, 2 * ff), rows)],
        out_shape=[
            jax.ShapeDtypeStruct((count, ff), jnp.bfloat16),
            jax.ShapeDtypeStruct((count, 2 * ff), jnp.bfloat16),
        ],
        compiler_params=pltpu.CompilerParams(vmem_limit_bytes=VMEM_MAX),
        cost_estimate=cost(6 * count * depth * ff, 4 * count * depth),
        name="mlp_middle",
    )(tokens, grads, w_gate, w_up, w_down)


rope_theta = 130000.0
norm_eps = 1e-05


def rotary_tables(position_list, width):
    half_dim = HD // 2
    frequency = rope_theta ** (-(jnp.arange(half_dim, dtype=jnp.float32) * 2.0 / HD))
    angles = position_list.astype(jnp.float32)[:, None] * frequency[None, :]
    cosine, sine = jnp.cos(angles), jnp.sin(angles)
    times = width // HD
    return (
        jnp.concatenate([cosine, cosine] * times, axis=1),
        jnp.concatenate([-sine, sine] * times, axis=1),
    )


def normalize(row_values):
    inverse = lax.rsqrt(jnp.mean(row_values * row_values, axis=-1, keepdims=True) + norm_eps)
    return (row_values * inverse, inverse)


def norm_back(grad_in, gain_vec, unit_rows, inverse):
    scaled = grad_in * gain_vec
    return inverse * (scaled - unit_rows * jnp.mean(scaled * unit_rows, axis=-1, keepdims=True))


def hop(piece, moves):
    return lax.ppermute(piece, "dp", moves)


def sum_over_dp(piece):
    if lax.axis_size("dp") != 4:
        return lax.psum(piece, "dp").astype(jnp.float32)
    place = lax.axis_index("dp")
    inner = (place == 1) | (place == 2)
    pair = piece + hop(piece, [(0, 1), (3, 2)])
    whole = pair + hop(pair, [(1, 2), (2, 1)])
    arrived = hop(whole, [(1, 0), (2, 3)])
    return jnp.where(inner, whole, arrived).astype(jnp.float32)


def local(
    layer_input,
    gain_attn,
    w_query,
    w_key,
    w_value,
    w_out,
    gain_mlp,
    w_gate,
    w_up,
    w_down,
    segment_ids,
    positions,
    out_grad,
):
    width = layer_input.shape[1]
    hidden_w = w_query.shape[1]
    ff_local = w_gate.shape[1]
    length = positions.shape[1]
    bf16, f32 = jnp.bfloat16, jnp.float32
    block = min(512, length)

    def gather(value):
        return lax.all_gather(value, "tensor", axis=0, tiled=True)

    def scatter(value):
        return lax.psum_scatter(value, "tensor", scatter_dimension=0, tiled=True)

    def mm(a, b, dims=(((1,), (0,)), ((), ()))):
        return lax.dot_general(a, b, dims, preferred_element_type=f32)

    TN = (((0,), (0,)), ((), ()))
    size = group_width(hidden_w)
    groups = range(hidden_w // size)
    group_w = [
        jnp.concatenate([w[:, g * size : (g + 1) * size] for w in (w_query, w_key, w_value)], axis=1)
        for g in groups
    ]
    joined_w = jnp.concatenate(group_w, axis=1)
    both_w = jnp.concatenate([w_gate, w_up], axis=1)
    cosine, sine = rotary_tables(positions.reshape(-1), size)

    inputs = layer_input.astype(f32)
    unit_one, inverse_one = normalize(inputs)
    all_one = gather((unit_one * gain_attn).astype(bf16))
    all_grad = gather(out_grad)
    all_w_out = gather(w_out)
    queries, keys, values = project(all_one, joined_w, cosine, sine)
    attended, level = attend_forward(queries, keys, values, positions, block, block)
    mixed = lax.all_to_all(attended, "tensor", split_axis=0, concat_axis=1, tiled=True)
    residual = inputs + mm(mixed, all_w_out)

    unit_two, inverse_two = normalize(residual)
    all_two = gather((unit_two * gain_mlp).astype(bf16))
    hidden, d_both = mlp_middle(all_two, all_grad, w_gate, w_up, w_down)
    half_ff, half = ff_local // 2, width // 2
    grad_down = [
        mm(hidden[:, :half_ff], all_grad, TN).astype(bf16),
        mm(hidden[:, half_ff:], all_grad, TN).astype(bf16),
    ]
    d_two = scatter(mm(d_both, both_w, NT).astype(bf16)).astype(f32)
    grad_gate = mm(all_two, d_both[:, :ff_local], TN).astype(bf16)
    grad_up = [
        mm(all_two[:, :half], d_both[:, ff_local:], TN).astype(bf16),
        mm(all_two[:, half:], d_both[:, ff_local:], TN).astype(bf16),
    ]
    layer_sum = scatter(mm(hidden, w_down).astype(bf16))

    gain_two_part = jnp.sum(d_two * unit_two, axis=0)
    d_residual = out_grad.astype(f32) + norm_back(d_two, gain_mlp, unit_two, inverse_two)
    d_attn = d_residual.astype(bf16)
    d_mixed = mm(d_attn, all_w_out, NT).astype(bf16)
    d_attended = lax.all_to_all(d_mixed, "tensor", split_axis=1, concat_axis=0, tiled=True)
    grad_out = mm(mixed, d_attn, TN).astype(bf16)
    d_attended, grad_out = lax.optimization_barrier((d_attended, grad_out))
    grad_out = scatter(grad_out)
    d_projected, grad_joined = [], []
    for g in groups:
        part = attend_backward(
            g, queries, keys, values, attended, d_attended, level, positions, cosine, sine,
            block, block,
        )
        d_projected.append(part)
        grad_joined.append(mm(all_one, part, TN).astype(bf16))
    layer_sum, last = lax.optimization_barrier((layer_sum, d_projected[-1]))
    d_projected = jnp.concatenate(d_projected[:-1] + [last], axis=1)
    layer_out = (residual + layer_sum.astype(f32)).astype(bf16)
    d_one = scatter(mm(d_projected, joined_w, NT).astype(bf16)).astype(f32)
    gain_one_part = sum(
        jnp.sum(grad.astype(f32) * w.astype(f32), axis=1)
        for grad, w in zip(lax.optimization_barrier(grad_joined), group_w)
    ) / gain_attn
    gains = lax.psum_scatter(
        jnp.stack([gain_one_part, gain_two_part]), "tensor", scatter_dimension=1, tiled=True
    )
    gains = sum_over_dp(gains)
    input_grad = d_residual + norm_back(d_one, gain_attn, unit_one, inverse_one)

    over_dp = lambda pieces: [sum_over_dp(p) for p in pieces]
    down = jnp.concatenate(over_dp(grad_down), axis=0)
    gate = sum_over_dp(grad_gate)
    up = jnp.concatenate(over_dp(grad_up), axis=0)
    joined = over_dp(grad_joined)
    out = sum_over_dp(grad_out)
    pick = lambda n: jnp.concatenate([part[:, n * size : (n + 1) * size] for part in joined], axis=1)
    return (
        layer_out,
        input_grad,
        gains[0],
        pick(0),
        pick(1),
        pick(2),
        out,
        gains[1],
        gate,
        up,
        down,
    )


def solution(mesh):
    return jax.shard_map(
        local,
        mesh=mesh,
        in_specs=(
            P(("dp", "tensor"), None),
            P(),
            P(None, "tensor"),
            P(None, "tensor"),
            P(None, "tensor"),
            P("tensor", None),
            P(),
            P(None, "tensor"),
            P(None, "tensor"),
            P("tensor", None),
            P("dp", None),
            P("dp", None),
            P(("dp", "tensor"), None),
        ),
        out_specs=(
            P(("dp", "tensor"), None),
            P(("dp", "tensor"), None),
            P("tensor"),
            P(None, "tensor"),
            P(None, "tensor"),
            P(None, "tensor"),
            P("tensor", None),
            P("tensor"),
            P(None, "tensor"),
            P(None, "tensor"),
            P("tensor", None),
        ),
        check_vma=False,
    )
```
